128 devices in a mesh: grp: 8 (over y, core), loc: 16 (over x, z).
Axes of the slice: x: 4, y: 4, z: 4, core: 2. Of those that a mesh axis runs over, the one named last changes fastest.
Arguments:
- tokens: bfloat16 [32768, 1024], P(('grp', 'loc')), may hold values from -6 to 6
- w_gate: bfloat16 [128, 1024, 2816], P(('grp', 'loc')), may hold values from -0.1875 to 0.1875
- w_up: bfloat16 [128, 1024, 2816], P(('grp', 'loc')), may hold values from -0.1875 to 0.1875
- w_down: bfloat16 [128, 2816, 1024], P(('grp', 'loc')), may hold values from -0.109375 to 0.109375
- chosen: int32 [128, 512], replicated, may hold values from -1 to 32767, as said below
- gate_weights: float32 [128, 512], replicated, may hold values from 0.05 to 1
Outputs:
- combined: bfloat16 [32768, 1024], P(('grp', 'loc'))
The draws below stay inside these ranges and needn't reach their ends.
Inputs may be any that keep to these rules, and one draw needn't show every extreme that they name: `chosen`: each entry is a token index or -1 for an empty slot, empty slots anywhere in a row. One expert's row names a token at most once. At most 8 entries of one expert's row lie among the 256 tokens of one device, and every expert has exactly 8 from some device. Some expert has no empty slot.
All inputs are finite; a program needn't handle non-finite values.
Results may differ from the reference program's by a relative error of at most 0.0085.
Values may be sent and summed in bfloat16 or wider, within the bound.
A program may use at most 128 MiB of HBM per device.

```python
import math
import jax
import jax.numpy as jnp
from jax import lax

D = 1024
FF = 2816
TOK_DEV = 256
PAIR_MOST = 8
EXPERTS = 128
CAP = 512
TOKENS = 32768


def draw_chosen(key, part):
    key_level, key_count, key_order, key_full, key_local, key_shuffle = jax.random.split(key, 6)
    load_level = jax.random.randint(key_level, (EXPERTS,), 0, 4)
    ceiling = jnp.minimum(jnp.array([5, 7, 9, 9], jnp.int32)[load_level], PAIR_MOST + 1)
    counts = jax.random.randint(key_count, (EXPERTS, EXPERTS), 0, ceiling[None, :])
    order_scores = jax.random.randint(key_order, (EXPERTS, EXPERTS), 0, 1 << 18) * EXPERTS + jnp.arange(EXPERTS)[None, :]
    source_order = jnp.argsort(order_scores, axis=1).astype(jnp.int32)
    ordered = jnp.take_along_axis(counts, source_order, axis=1)
    full_expert = jax.random.randint(key_full, (), 0, EXPERTS)
    row_iota = jnp.arange(EXPERTS)[:, None]
    column_iota = jnp.arange(EXPERTS)[None, :]
    ordered = jnp.where((column_iota == 0) | (row_iota == full_expert), PAIR_MOST, ordered)
    before = jnp.cumsum(ordered, axis=1) - ordered
    kept_count = jnp.minimum(jnp.maximum(CAP - before, 0), ordered)
    scores = jax.random.randint(key_local, (EXPERTS, EXPERTS, TOK_DEV), 0, 1 << 18) * TOK_DEV + jnp.arange(TOK_DEV)[None, None, :]
    local_pick = jnp.argsort(scores, axis=2)[:, :, :PAIR_MOST].astype(jnp.int32)
    global_id = source_order[:, :, None] * TOK_DEV + local_pick
    pair_iota = jnp.arange(PAIR_MOST)[None, None, :]
    is_valid = pair_iota < kept_count[:, :, None]
    slot_index = jnp.where(is_valid, before[:, :, None] + pair_iota, CAP)
    expert_ids = jnp.broadcast_to(row_iota[:, :, None], slot_index.shape)
    slot_table = jnp.full((EXPERTS, CAP), -1, jnp.int32).at[expert_ids, slot_index].set(global_id.astype(jnp.int32), mode='drop')
    shuffle_scores = jax.random.randint(key_shuffle, (EXPERTS, CAP), 0, 1 << 18) * CAP + jnp.arange(CAP)[None, :]
    shuffle = jnp.argsort(shuffle_scores, axis=1)
    return jnp.take_along_axis(slot_table, shuffle, axis=1)


def block_scale(key, dims, pieces, least, top_value):
    def one(axis_at, blocks):
        steps = jax.random.uniform(jax.random.fold_in(jax.random.fold_in(key, 6), axis_at), (blocks,), jnp.float32, least / len(pieces), top_value / len(pieces))
        return jnp.repeat(jnp.exp(steps), dims[axis_at] // blocks).reshape((-1,) + (1,) * (len(dims) - axis_at - 1))

    loudness = one(*pieces[0])
    for cut in pieces[1:]:
        loudness = loudness * one(*cut)
    return loudness


def centred(stream_key, dims, scale, most, cuts=(), kind=jnp.bfloat16):
    gain = block_scale(stream_key, dims, cuts, -0.22, 0.18) if cuts else 1.0
    drawn = jax.random.normal(stream_key, dims, jnp.float32) * scale * gain
    return jnp.minimum(jnp.maximum(drawn, -most), most).astype(kind)


def setup_inputs(seed: int = 0) -> dict:
    splits = jax.random.split(jax.random.key(seed), 7)
    return {
        "tokens": centred(splits[0], (TOKENS, D), 1.0, 6.0, ((0, 128),)),
        "w_gate": centred(splits[1], (EXPERTS, D, FF), D ** -0.5, 0.1875, ((0, 128),)),
        "w_up": centred(splits[2], (EXPERTS, D, FF), D ** -0.5, 0.1875, ((0, 128),)),
        "w_down": centred(splits[3], (EXPERTS, FF, D), FF ** -0.5, 0.109375, ((0, 128),)),
        "chosen": draw_chosen(jax.random.fold_in(splits[6], 71), 0),
        "gate_weights": jnp.clip(jnp.exp(jax.random.uniform(splits[5], (EXPERTS, CAP), jnp.float32, math.log(0.05), math.log(1.0))), 0.05, 1.0),
    }


def reference(tokens, w_gate, w_up, w_down, chosen, gate_weights):
    token_total = tokens.shape[0]
    model_width = tokens.shape[1]
    padded = jnp.concatenate([tokens, jnp.zeros((1, model_width), tokens.dtype)], axis=0)

    def one_expert(expert, running):
        picks = lax.dynamic_index_in_dim(chosen, expert, 0, keepdims=False)
        is_live = picks >= 0
        row_index = jnp.where(is_live, picks, token_total).astype(jnp.int32)
        row_block = jnp.take(padded, row_index, axis=0)
        gate_mat = lax.dynamic_index_in_dim(w_gate, expert, 0, keepdims=False)
        up_mat = lax.dynamic_index_in_dim(w_up, expert, 0, keepdims=False)
        down_mat = lax.dynamic_index_in_dim(w_down, expert, 0, keepdims=False)
        gate_pre = jnp.dot(row_block, gate_mat, preferred_element_type=jnp.float32)
        up_pre = jnp.dot(row_block, up_mat, preferred_element_type=jnp.float32)
        hidden = (jax.nn.silu(gate_pre) * up_pre).astype(jnp.bfloat16)
        expert_out = jnp.dot(hidden, down_mat, preferred_element_type=jnp.float32).astype(jnp.bfloat16)
        slot_weight = jnp.where(is_live, lax.dynamic_index_in_dim(gate_weights, expert, 0, keepdims=False), 0.0)
        weighted = slot_weight[:, None] * expert_out.astype(jnp.float32)
        return running.at[row_index].add(weighted)

    running = jnp.zeros((token_total + 1, model_width), jnp.float32)
    running = lax.fori_loop(0, EXPERTS, one_expert, running)
    return running[:token_total].astype(jnp.bfloat16)
```

```python
import jax
import jax.numpy as jnp
from jax import lax
from jax.experimental import pallas as pl
from jax.experimental.pallas import tpu as pltpu
from jax.sharding import PartitionSpec as P

PAIR = 8
SUB = 16
FF_TILES = ((0, 1024), (1024, 1024), (2048, 768))
MESH = pl.DeviceIdType.MESH
BF = jnp.bfloat16
F32 = jnp.float32


def partners(c, d, sign):
    g, l = lax.axis_index("grp"), lax.axis_index("loc")
    y, core = lax.div(g, 2), lax.rem(g, 2)
    x, z = lax.div(l, 4), lax.rem(l, 4)
    core2 = lax.rem(core + d, 2)
    if sign > 0:
        ys = [lax.rem(y + j, 4) * 2 + core2 for j in range(4)]
        xs = [lax.rem(x + j, 4) * 4 for j in range(4)]
        zs = [lax.rem(z + c + j, 4) for j in range(4)]
    else:
        ys = [lax.rem(y + 4 - j, 4) * 2 + core2 for j in range(4)]
        xs = [lax.rem(x + 4 - j, 4) * 4 for j in range(4)]
        zs = [lax.rem(z + 8 - c - j, 4) for j in range(4)]
    return [(ys[(a + b) % 4], xs[a] + zs[a]) for b in range(4) for a in range(4)]


def body(
    tokens_hbm, wg_hbm, wu_hbm, wd_hbm, chosen_hbm, weight_hbm, out_ref,
    tokens, wg, wu, wd, chosen, gates, upper, key, local, key2, select, spread, scale,
    send, recv, back, home, hidden, acc,
    in_sems, send_sem, recv_sems, back_sem, home_sems,
):
    n_dev, slots = chosen.shape
    n_tok, width = tokens.shape
    n_sub = n_dev // SUB
    rows = SUB * PAIR
    me = lax.axis_index("grp") * lax.axis_size("loc") + lax.axis_index("loc")

    def blocks(fn, sign):
        def step(s, _):
            d = lax.div(s, 4)
            fn(s, partners(s - 4 * d, d, sign))
            return 0

        lax.fori_loop(0, n_sub, step, 0)

    def skip_self(s, i, fn):
        if i == 0:
            pl.when(s > 0)(fn)
        else:
            fn()

    barrier = pltpu.get_barrier_semaphore()

    def greet(s, who):
        for i, w in enumerate(who):
            skip_self(s, i, lambda w=w: pl.semaphore_signal(barrier, inc=1, device_id=w, device_id_type=MESH))

    blocks(greet, 1)
    loads = [
        pltpu.make_async_copy(a, b, in_sems.at[i])
        for i, (a, b) in enumerate(
            ((chosen_hbm, chosen), (tokens_hbm, tokens), (weight_hbm, gates), (wg_hbm.at[0], wg), (wu_hbm.at[0], wu), (wd_hbm.at[0], wd))
        )
    ]
    for cp in loads:
        cp.start()

    row_i = lax.broadcasted_iota(jnp.int32, (slots, slots), 0)
    col_i = lax.broadcasted_iota(jnp.int32, (slots, slots), 1)
    upper[...] = jnp.where(row_i < col_i, 1.0, 0.0).astype(BF)
    pair_i = lax.broadcasted_iota(jnp.int32, (PAIR, slots), 0).astype(F32)
    token_i = (lax.broadcasted_iota(jnp.int32, (PAIR, n_tok), 1) + 1).astype(F32)

    def ranked(hit):
        ahead = jnp.dot(hit.astype(BF), upper[...], preferred_element_type=F32)
        return jnp.where(hit > 0.5, ahead, -1.0)

    loads[0].wait()
    picks = chosen[...]
    off = picks - me * n_tok
    mine = jnp.where((off >= 0) & (off < n_tok), 1.0, 0.0)
    key[...] = ranked(mine)
    local[...] = (off + 1).astype(F32)
    loads[1].wait()

    def build(s, who):
        for i, (g, l) in enumerate(who):
            e = g * lax.axis_size("loc") + l
            hit = key[pl.ds(e, 1), :] == pair_i
            where = jnp.sum(jnp.where(hit, local[pl.ds(e, 1), :], 0.0), axis=1, keepdims=True)
            select[pl.ds(pl.multiple_of(s * rows, rows) + i * PAIR, PAIR), :] = jnp.where(token_i == where, 1.0, 0.0)

    blocks(build, 1)

    def gather(s, _):
        block = select[pl.ds(pl.multiple_of(s * rows, rows), rows), :].astype(BF)
        picked = jnp.dot(block, tokens[...], preferred_element_type=F32)
        send[pl.ds(s * SUB, SUB)] = picked.reshape(SUB, PAIR, width).astype(BF)
        return 0

    lax.fori_loop(0, n_sub, gather, 0)
    recv[0] = send[0]
    pl.semaphore_wait(barrier, n_dev - 1)

    def dispatch(s, who):
        for i, w in enumerate(who):
            k = s * SUB + i
            skip_self(
                s, i,
                lambda k=k, w=w: pltpu.make_async_remote_copy(
                    send.at[k], recv.at[k], send_sem, recv_sems.at[s], device_id=w, device_id_type=MESH
                ).start(),
            )

    blocks(dispatch, 1)

    for s in range(n_sub):
        spread[:, s * rows : (s + 1) * rows] = select[s * rows : (s + 1) * rows, :].T.astype(BF)
    own = jnp.broadcast_to(chosen[pl.ds(me, 1), :], (n_dev, slots))
    low = lax.broadcasted_iota(jnp.int32, (n_dev, slots), 0) * n_tok
    key2[...] = ranked(jnp.where((own >= low) & (own < low + n_tok), 1.0, 0.0))
    loads[2].wait()
    own_gate = gates[pl.ds(me, 1), :]

    def weigh(s, who):
        for i, (g, l) in enumerate(who):
            e = g * lax.axis_size("loc") + l
            hit = key2[pl.ds(e, 1), :] == pair_i
            value = jnp.sum(jnp.where(hit, own_gate, 0.0), axis=1, keepdims=True)
            scale[pl.ds(pl.multiple_of(s * rows, rows) + i * PAIR, PAIR), :] = jnp.broadcast_to(value, (PAIR, scale.shape[1]))

    blocks(weigh, -1)
    for cp in loads[3:]:
        cp.wait()

    def got(sems, buf, s):
        @pl.when(s == 0)
        def _():
            ref = buf.at[pl.ds(1, SUB - 1)]
            pltpu.make_async_copy(ref, ref, sems.at[0]).wait()

        @pl.when(s > 0)
        def _():
            ref = buf.at[pl.ds(s * SUB, SUB)]
            pltpu.make_async_copy(ref, ref, sems.at[s]).wait()

    def expert(s, who):
        got(recv_sems, recv, s)
        x = recv[pl.ds(s * SUB, SUB)].astype(F32).reshape(rows, width).astype(BF)
        for start, size in FF_TILES:
            gate = jnp.dot(x, wg[:, start : start + size], preferred_element_type=F32)
            up = jnp.dot(x, wu[:, start : start + size], preferred_element_type=F32)
            hidden[:, start : start + size] = (gate / (1.0 + jnp.exp(-gate)) * up).astype(BF)
        made = jnp.dot(hidden[...], wd[...], preferred_element_type=F32)
        made = made * scale[pl.ds(pl.multiple_of(s * rows, rows), rows), :1]
        back[pl.ds(s * SUB, SUB)] = made.reshape(SUB, PAIR, width).astype(BF)
        for i, w in enumerate(who):
            k = s * SUB + i
            skip_self(
                s, i,
                lambda k=k, w=w: pltpu.make_async_remote_copy(
                    back.at[k], home.at[k], back_sem, home_sems.at[s], device_id=w, device_id_type=MESH
                ).start(),
            )

    blocks(expert, -1)
    home[0] = back[0]
    acc[...] = jnp.zeros_like(acc)

    def combine(s, _):
        got(home_sems, home, s)
        r = home[pl.ds(s * SUB, SUB)].astype(F32).reshape(rows, width).astype(BF)
        acc[...] += jnp.dot(spread[:, pl.ds(pl.multiple_of(s * rows, rows), rows)], r, preferred_element_type=F32)
        return 0

    lax.fori_loop(0, n_sub, combine, 0)
    out_ref[...] = acc[...].astype(out_ref.dtype)
    sent = send.at[pl.ds(1, n_dev - 1)]
    pltpu.make_async_copy(sent, sent, send_sem).wait()
    sent = back.at[pl.ds(1, n_dev - 1)]
    pltpu.make_async_copy(sent, sent, back_sem).wait()


def shards(tokens, w_gate, w_up, w_down, chosen, gate_weights):
    n_tok, width = tokens.shape
    n_dev, slots = chosen.shape
    ff = w_gate.shape[2]
    n_sub = n_dev // SUB
    any_space = pl.BlockSpec(memory_space=pl.ANY)
    total = n_dev * PAIR
    return pl.pallas_call(
        body,
        out_shape=jax.ShapeDtypeStruct((n_tok, width), BF),
        in_specs=[any_space] * 6,
        out_specs=pl.BlockSpec(memory_space=pltpu.VMEM),
        scratch_shapes=[
            pltpu.VMEM((n_tok, width), BF),
            pltpu.VMEM((width, ff), BF),
            pltpu.VMEM((width, ff), BF),
            pltpu.VMEM((ff, width), BF),
            pltpu.VMEM((n_dev, slots), jnp.int32),
            pltpu.VMEM((n_dev, slots), F32),
            pltpu.VMEM((slots, slots), BF),
            pltpu.VMEM((n_dev, slots), F32),
            pltpu.VMEM((n_dev, slots), F32),
            pltpu.VMEM((n_dev, slots), F32),
            pltpu.VMEM((total, n_tok), F32),
            pltpu.VMEM((n_tok, total), BF),
            pltpu.VMEM((total, 128), F32),
            pltpu.VMEM((n_dev, PAIR, width), BF),
            pltpu.VMEM((n_dev, PAIR, width), BF),
            pltpu.VMEM((n_dev, PAIR, width), BF),
            pltpu.VMEM((n_dev, PAIR, width), BF),
            pltpu.VMEM((SUB * PAIR, ff), BF),
            pltpu.VMEM((n_tok, width), F32),
            pltpu.SemaphoreType.DMA((6,)),
            pltpu.SemaphoreType.DMA,
            pltpu.SemaphoreType.DMA((n_sub,)),
            pltpu.SemaphoreType.DMA,
            pltpu.SemaphoreType.DMA((n_sub,)),
        ],
        compiler_params=pltpu.CompilerParams(
            collective_id=0, has_side_effects=True, vmem_limit_bytes=56 << 20
        ),
    )(tokens, w_gate, w_up, w_down, chosen, gate_weights)


def solution(mesh):
    return jax.shard_map(
        shards,
        mesh=mesh,
        in_specs=(
            P(("grp", "loc"), None),
            P(("grp", "loc"), None, None),
            P(("grp", "loc"), None, None),
            P(("grp", "loc"), None, None),
            P(),
            P(),
        ),
        out_specs=P(("grp", "loc"), None),
        check_vma=False,
    )
```

```python
import itertools

import jax
import jax.numpy as jnp
from jax import lax
from jax.experimental import pallas as pl
from jax.experimental.pallas import tpu as pltpu
from jax.sharding import PartitionSpec as P

PAIR = 8
SUB = 16
FF_TILES = ((0, 1024), (1024, 1024), (2048, 768))
MESH = pl.DeviceIdType.MESH
BF = jnp.bfloat16
F32 = jnp.float32


def by_link_load(offsets):
    loads = {}
    for o in offsets:
        hops = []
        for d in (o[0], o[2], o[3]):
            hops += [1.0 if d in (1, 2) else 0.0, 1.0 if d in (2, 3) else 0.0]
        loads[o] = hops
    total = [sum(loads[o][i] for o in offsets) for i in range(6)]
    left, done, out = list(offsets), [0.0] * 6, []
    for n in range(len(offsets)):
        goal = [(n + 1) * t / len(offsets) for t in total]
        best = min(left, key=lambda o: sum((a + b - g) ** 2 for a, b, g in zip(done, loads[o], goal)))
        done = [a + b for a, b in zip(done, loads[best])]
        left.remove(best)
        out.append(best)
    return out


OTHERS = [o for o in itertools.product(range(4), range(2), range(4), range(4)) if any(o)]
ORDER = [(0, 0, 0, 0)] + by_link_load(OTHERS)


def hops(o):
    return sum(min(d, 4 - d) for d in (o[0], o[2], o[3]))


def body(
    tokens_hbm, wg_hbm, wu_hbm, wd_hbm, chosen_hbm, weight_hbm, out_ref,
    tokens, wg, wu, wd, chosen, gates, upper, key, local, key2, select, spread, scale,
    send, recv, back, home, hidden, acc,
    in_sems, send_sem, recv_sems, back_sem, home_sems,
):
    n_dev, slots = chosen.shape
    n_tok, width = tokens.shape
    n_sub = n_dev // SUB
    rows = SUB * PAIR
    me = lax.axis_index("grp") * lax.axis_size("loc") + lax.axis_index("loc")
    g, l = lax.axis_index("grp"), lax.axis_index("loc")
    ys = [lax.rem(lax.div(g, 2) + j, 4) * 2 for j in range(4)]
    cores = [lax.rem(g + j, 2) for j in range(2)]
    xs = [lax.rem(lax.div(l, 4) + j, 4) * 4 for j in range(4)]
    zs = [lax.rem(lax.rem(l, 4) + j, 4) for j in range(4)]

    def partner(o, sign):
        dy, dc, dx, dz = o
        return ys[(sign * dy) % 4] + cores[dc], xs[(sign * dx) % 4] + zs[(sign * dz) % 4]

    barrier = pltpu.get_barrier_semaphore()
    for o in sorted(OTHERS, key=hops, reverse=True):
        pl.semaphore_signal(barrier, inc=1, device_id=partner(o, 1), device_id_type=MESH)
    loads = [
        pltpu.make_async_copy(a, b, in_sems.at[i])
        for i, (a, b) in enumerate(
            ((chosen_hbm, chosen), (tokens_hbm, tokens), (weight_hbm, gates), (wg_hbm.at[0], wg), (wu_hbm.at[0], wu), (wd_hbm.at[0], wd))
        )
    ]
    for cp in loads:
        cp.start()

    row_i = lax.broadcasted_iota(jnp.int32, (slots, slots), 0)
    col_i = lax.broadcasted_iota(jnp.int32, (slots, slots), 1)
    upper[...] = jnp.where(row_i < col_i, 1.0, 0.0).astype(BF)
    pair_i = lax.broadcasted_iota(jnp.int32, (PAIR, slots), 0).astype(F32)
    token_i = (lax.broadcasted_iota(jnp.int32, (PAIR, n_tok), 1) + 1).astype(F32)

    def ranked(hit):
        ahead = jnp.dot(hit.astype(BF), upper[...], preferred_element_type=F32)
        return jnp.where(hit > 0.5, ahead, -1.0)

    loads[0].wait()
    picks = chosen[...]
    off = picks - me * n_tok
    mine = jnp.where((off >= 0) & (off < n_tok), 1.0, 0.0)
    key[...] = ranked(mine)
    local[...] = (off + 1).astype(F32)
    loads[1].wait()

    def build(s):
        for k in range(s * SUB, (s + 1) * SUB):
            pg, pl_ = partner(ORDER[k], 1)
            e = pg * lax.axis_size("loc") + pl_
            hit = key[pl.ds(e, 1), :] == pair_i
            where = jnp.sum(jnp.where(hit, local[pl.ds(e, 1), :], 0.0), axis=1, keepdims=True)
            select[k * PAIR : (k + 1) * PAIR, :] = jnp.where(token_i == where, 1.0, 0.0)
        block = select[s * rows : (s + 1) * rows, :].astype(BF)
        picked = jnp.dot(block, tokens[...], preferred_element_type=F32)
        send[s * SUB : (s + 1) * SUB] = picked.reshape(SUB, PAIR, width).astype(BF)

    def dispatch(first, last):
        for k in range(first, last):
            pltpu.make_async_remote_copy(
                send.at[k], recv.at[k], send_sem, recv_sems.at[k // SUB],
                device_id=partner(ORDER[k], 1), device_id_type=MESH,
            ).start()

    build(0)
    recv[0] = send[0]
    pl.semaphore_wait(barrier, n_dev - 1)
    dispatch(1, SUB)
    for s in range(1, n_sub):
        build(s)
        dispatch(s * SUB, (s + 1) * SUB)

    for s in range(n_sub):
        spread[:, s * rows : (s + 1) * rows] = select[s * rows : (s + 1) * rows, :].T.astype(BF)
    own = jnp.broadcast_to(chosen[pl.ds(me, 1), :], (n_dev, slots))
    low = lax.broadcasted_iota(jnp.int32, (n_dev, slots), 0) * n_tok
    key2[...] = ranked(jnp.where((own >= low) & (own < low + n_tok), 1.0, 0.0))
    loads[2].wait()
    own_gate = gates[pl.ds(me, 1), :]

    for k in range(n_dev):
        pg, pl_ = partner(ORDER[k], -1)
        e = pg * lax.axis_size("loc") + pl_
        hit = key2[pl.ds(e, 1), :] == pair_i
        value = jnp.sum(jnp.where(hit, own_gate, 0.0), axis=1, keepdims=True)
        scale[k * PAIR : (k + 1) * PAIR, :] = jnp.broadcast_to(value, (PAIR, scale.shape[1]))

    for cp in loads[3:]:
        cp.wait()

    def got(sems, buf, s):
        @pl.when(s == 0)
        def _():
            ref = buf.at[pl.ds(1, SUB - 1)]
            pltpu.make_async_copy(ref, ref, sems.at[0]).wait()

        @pl.when(s > 0)
        def _():
            ref = buf.at[pl.ds(s * SUB, SUB)]
            pltpu.make_async_copy(ref, ref, sems.at[s]).wait()

    def expert(s, _):
        got(recv_sems, recv, s)
        x = recv[pl.ds(s * SUB, SUB)].astype(F32).reshape(rows, width).astype(BF)
        for start, size in FF_TILES:
            gate = jnp.dot(x, wg[:, start : start + size], preferred_element_type=F32)
            up = jnp.dot(x, wu[:, start : start + size], preferred_element_type=F32)
            hidden[:, start : start + size] = (gate / (1.0 + jnp.exp(-gate)) * up).astype(BF)
        made = jnp.dot(hidden[...], wd[...], preferred_element_type=F32)
        made = made * scale[pl.ds(pl.multiple_of(s * rows, rows), rows), :1]
        back[pl.ds(s * SUB, SUB)] = made.reshape(SUB, PAIR, width).astype(BF)
        for j in range(n_sub):

            @pl.when(s == j)
            def _():
                for k in range(max(j * SUB, 1), (j + 1) * SUB):
                    pltpu.make_async_remote_copy(
                        back.at[k], home.at[k], back_sem, home_sems.at[j],
                        device_id=partner(ORDER[k], -1), device_id_type=MESH,
                    ).start()

        return 0

    lax.fori_loop(0, n_sub, expert, 0)
    home[0] = back[0]
    acc[...] = jnp.zeros_like(acc)

    def part(s):
        got(home_sems, home, s)
        r = home[pl.ds(s * SUB, SUB)].astype(F32).reshape(rows, width).astype(BF)
        table = spread[:, pl.ds(pl.multiple_of(s * rows, rows), rows)]
        return jnp.dot(table, r, preferred_element_type=F32)

    def combine(s, _):
        acc[...] += part(s)
        return 0

    lax.fori_loop(0, n_sub - 1, combine, 0)
    out_ref[...] = (acc[...] + part(n_sub - 1)).astype(out_ref.dtype)
    sent = send.at[pl.ds(1, n_dev - 1)]
    pltpu.make_async_copy(sent, sent, send_sem).wait()
    sent = back.at[pl.ds(1, n_dev - 1)]
    pltpu.make_async_copy(sent, sent, back_sem).wait()


def shards(tokens, w_gate, w_up, w_down, chosen, gate_weights):
    n_tok, width = tokens.shape
    n_dev, slots = chosen.shape
    ff = w_gate.shape[2]
    n_sub = n_dev // SUB
    total = n_dev * PAIR
    return pl.pallas_call(
        body,
        out_shape=pltpu.VMEM((n_tok, width), BF),
        in_specs=[pl.BlockSpec(memory_space=pltpu.HBM)] * 6,
        out_specs=pl.BlockSpec(memory_space=pltpu.VMEM),
        scratch_shapes=[
            pltpu.VMEM((n_tok, width), BF),
            pltpu.VMEM((width, ff), BF),
            pltpu.VMEM((width, ff), BF),
            pltpu.VMEM((ff, width), BF),
            pltpu.VMEM((n_dev, slots), jnp.int32),
            pltpu.VMEM((n_dev, slots), F32),
            pltpu.VMEM((slots, slots), BF),
            pltpu.VMEM((n_dev, slots), F32),
            pltpu.VMEM((n_dev, slots), F32),
            pltpu.VMEM((n_dev, slots), F32),
            pltpu.VMEM((total, n_tok), F32),
            pltpu.VMEM((n_tok, total), BF),
            pltpu.VMEM((total, 128), F32),
            pltpu.VMEM((n_dev, PAIR, width), BF),
            pltpu.VMEM((n_dev, PAIR, width), BF),
            pltpu.VMEM((n_dev, PAIR, width), BF),
            pltpu.VMEM((n_dev, PAIR, width), BF),
            pltpu.VMEM((SUB * PAIR, ff), BF),
            pltpu.VMEM((n_tok, width), F32),
            pltpu.SemaphoreType.DMA((6,)),
            pltpu.SemaphoreType.DMA,
            pltpu.SemaphoreType.DMA((n_sub,)),
            pltpu.SemaphoreType.DMA,
            pltpu.SemaphoreType.DMA((n_sub,)),
        ],
        compiler_params=pltpu.CompilerParams(
            collective_id=0, has_side_effects=True, vmem_limit_bytes=56 << 20
        ),
    )(tokens, w_gate, w_up, w_down, chosen, gate_weights)


def solution(mesh):
    return jax.shard_map(
        shards,
        mesh=mesh,
        in_specs=(
            P(("grp", "loc"), None),
            P(("grp", "loc"), None, None),
            P(("grp", "loc"), None, None),
            P(("grp", "loc"), None, None),
            P(),
            P(),
        ),
        out_specs=P(("grp", "loc"), None),
        check_vma=False,
    )
```

```python
import itertools

import jax
import jax.numpy as jnp
from jax import lax
from jax.experimental import pallas as pl
from jax.experimental.pallas import tpu as pltpu
from jax.sharding import PartitionSpec as P

N_FIRST = 19
PAIR = 8
SUB = 16
FF_TILES = ((0, 1024), (1024, 1024), (2048, 768))
MESH = pl.DeviceIdType.MESH
BF = jnp.bfloat16
F32 = jnp.float32


def by_link_load(offsets):
    loads = {}
    for o in offsets:
        hops = []
        for d in (o[0], o[2], o[3]):
            hops += [1.0 if d in (1, 2) else 0.0, 1.0 if d in (2, 3) else 0.0]
        loads[o] = hops
    total = [sum(loads[o][i] for o in offsets) for i in range(6)]
    left, done, out = list(offsets), [0.0] * 6, []
    for n in range(len(offsets)):
        goal = [(n + 1) * t / len(offsets) for t in total]
        best = min(left, key=lambda o: sum((a + b - g) ** 2 for a, b, g in zip(done, loads[o], goal)))
        done = [a + b for a, b in zip(done, loads[best])]
        left.remove(best)
        out.append(best)
    return out


OTHERS = [o for o in itertools.product(range(4), range(2), range(4), range(4)) if any(o)]


def lines_left(o):
    return (o[:2] != (0, 0)) + (o[2] > 0) + (o[3] > 0)


NEAR = [o for o in OTHERS if lines_left(o) < 3]
X_LINE = [o for o in OTHERS if o[2] > 0 and lines_left(o) == 1]
FIRST = by_link_load(sorted(NEAR, key=lines_left)[:N_FIRST])
ORDER = [(0, 0, 0, 0)] + FIRST + by_link_load([o for o in OTHERS if o not in FIRST])


def hops(o):
    return sum(min(d, 4 - d) for d in (o[0], o[2], o[3]))


def body(
    tokens_hbm, wg_hbm, wu_hbm, wd_hbm, chosen_hbm, weight_hbm, out_ref,
    tokens, wg, wu, wd, chosen, gates, upper, key, local, key2, select, spread, scale,
    send, recv, back, home, hidden, acc,
    in_sems, send_sem, recv_sems, back_sem, home_sems, far_sem,
):
    n_dev, slots = chosen.shape
    n_tok, width = tokens.shape
    n_sub = n_dev // SUB
    rows = SUB * PAIR
    me = lax.axis_index("grp") * lax.axis_size("loc") + lax.axis_index("loc")
    g, l = lax.axis_index("grp"), lax.axis_index("loc")
    ys = [lax.rem(lax.div(g, 2) + j, 4) * 2 for j in range(4)]
    cores = [lax.rem(g + j, 2) for j in range(2)]
    xs = [lax.rem(lax.div(l, 4) + j, 4) * 4 for j in range(4)]
    zs = [lax.rem(lax.rem(l, 4) + j, 4) for j in range(4)]

    def partner(o, sign):
        dy, dc, dx, dz = o
        return ys[(sign * dy) % 4] + cores[dc], xs[(sign * dx) % 4] + zs[(sign * dz) % 4]

    barrier = pltpu.get_barrier_semaphore()
    for o in sorted(NEAR, key=hops, reverse=True):
        pl.semaphore_signal(barrier, inc=1, device_id=partner(o, 1), device_id_type=MESH)
    loads = [
        pltpu.make_async_copy(a, b, in_sems.at[i])
        for i, (a, b) in enumerate(
            ((chosen_hbm, chosen), (tokens_hbm, tokens), (weight_hbm, gates), (wg_hbm.at[0], wg), (wu_hbm.at[0], wu), (wd_hbm.at[0], wd))
        )
    ]
    for cp in loads:
        cp.start()

    row_i = lax.broadcasted_iota(jnp.int32, (slots, slots), 0)
    col_i = lax.broadcasted_iota(jnp.int32, (slots, slots), 1)
    upper[...] = jnp.where(row_i < col_i, 1.0, 0.0).astype(BF)
    pair_i = lax.broadcasted_iota(jnp.int32, (PAIR, slots), 0).astype(F32)
    token_i = (lax.broadcasted_iota(jnp.int32, (PAIR, n_tok), 1) + 1).astype(F32)

    def ranked(hit):
        ahead = jnp.dot(hit.astype(BF), upper[...], preferred_element_type=F32)
        return jnp.where(hit > 0.5, ahead, -1.0)

    loads[0].wait()
    picks = chosen[...]
    off = picks - me * n_tok
    mine = jnp.where((off >= 0) & (off < n_tok), 1.0, 0.0)
    key[...] = ranked(mine)
    local[...] = (off + 1).astype(F32)
    loads[1].wait()

    def build(s):
        for k in range(s * SUB, (s + 1) * SUB):
            pg, pl_ = partner(ORDER[k], 1)
            e = pg * lax.axis_size("loc") + pl_
            hit = key[pl.ds(e, 1), :] == pair_i
            where = jnp.sum(jnp.where(hit, local[pl.ds(e, 1), :], 0.0), axis=1, keepdims=True)
            select[k * PAIR : (k + 1) * PAIR, :] = jnp.where(token_i == where, 1.0, 0.0)
        block = select[s * rows : (s + 1) * rows, :].astype(BF)
        picked = jnp.dot(block, tokens[...], preferred_element_type=F32)
        send[s * SUB : (s + 1) * SUB] = picked.reshape(SUB, PAIR, width).astype(BF)

    def dispatch(first, last):
        for k in range(first, last):
            pltpu.make_async_remote_copy(
                send.at[k], recv.at[k], send_sem, recv_sems.at[k // SUB],
                device_id=partner(ORDER[k], 1), device_id_type=MESH,
            ).start()

    build(0)
    recv[0] = send[0]
    pl.semaphore_wait(barrier, len(NEAR))
    for o in X_LINE:
        pl.semaphore_signal(far_sem, inc=1, device_id=partner(o, 1), device_id_type=MESH)
    dispatch(1, SUB)
    for s in range(1, n_sub):
        build(s)
        first, last, known = s * SUB, (s + 1) * SUB, len(FIRST) + 1
        if first <= known < last:
            dispatch(first, known)
            pl.semaphore_wait(far_sem, len(X_LINE))
            first = known
        dispatch(first, last)

    for s in range(n_sub):
        spread[:, s * rows : (s + 1) * rows] = select[s * rows : (s + 1) * rows, :].T.astype(BF)
    own = jnp.broadcast_to(chosen[pl.ds(me, 1), :], (n_dev, slots))
    low = lax.broadcasted_iota(jnp.int32, (n_dev, slots), 0) * n_tok
    key2[...] = ranked(jnp.where((own >= low) & (own < low + n_tok), 1.0, 0.0))
    loads[2].wait()
    own_gate = gates[pl.ds(me, 1), :]

    for k in range(n_dev):
        pg, pl_ = partner(ORDER[k], -1)
        e = pg * lax.axis_size("loc") + pl_
        hit = key2[pl.ds(e, 1), :] == pair_i
        value = jnp.sum(jnp.where(hit, own_gate, 0.0), axis=1, keepdims=True)
        scale[k * PAIR : (k + 1) * PAIR, :] = jnp.broadcast_to(value, (PAIR, scale.shape[1]))

    for cp in loads[3:]:
        cp.wait()

    def got(sems, buf, s):
        @pl.when(s == 0)
        def _():
            ref = buf.at[pl.ds(1, SUB - 1)]
            pltpu.make_async_copy(ref, ref, sems.at[0]).wait()

        @pl.when(s > 0)
        def _():
            ref = buf.at[pl.ds(s * SUB, SUB)]
            pltpu.make_async_copy(ref, ref, sems.at[s]).wait()

    def expert(s, _):
        got(recv_sems, recv, s)
        x = recv[pl.ds(s * SUB, SUB)].astype(F32).reshape(rows, width).astype(BF)
        for start, size in FF_TILES:
            gate = jnp.dot(x, wg[:, start : start + size], preferred_element_type=F32)
            up = jnp.dot(x, wu[:, start : start + size], preferred_element_type=F32)
            hidden[:, start : start + size] = (gate / (1.0 + jnp.exp(-gate)) * up).astype(BF)
        made = jnp.dot(hidden[...], wd[...], preferred_element_type=F32)
        made = made * scale[pl.ds(pl.multiple_of(s * rows, rows), rows), :1]
        back[pl.ds(s * SUB, SUB)] = made.reshape(SUB, PAIR, width).astype(BF)
        for j in range(n_sub):

            @pl.when(s == j)
            def _():
                for k in range(max(j * SUB, 1), (j + 1) * SUB):
                    pltpu.make_async_remote_copy(
                        back.at[k], home.at[k], back_sem, home_sems.at[j],
                        device_id=partner(ORDER[k], -1), device_id_type=MESH,
                    ).start()

        return 0

    lax.fori_loop(0, n_sub, expert, 0)
    home[0] = back[0]
    acc[...] = jnp.zeros_like(acc)

    def part(s):
        got(home_sems, home, s)
        r = home[pl.ds(s * SUB, SUB)].astype(F32).reshape(rows, width).astype(BF)
        table = spread[:, pl.ds(pl.multiple_of(s * rows, rows), rows)]
        return jnp.dot(table, r, preferred_element_type=F32)

    def combine(s, _):
        acc[...] += part(s)
        return 0

    lax.fori_loop(0, n_sub - 1, combine, 0)
    out_ref[...] = (acc[...] + part(n_sub - 1)).astype(out_ref.dtype)
    sent = send.at[pl.ds(1, n_dev - 1)]
    pltpu.make_async_copy(sent, sent, send_sem).wait()
    sent = back.at[pl.ds(1, n_dev - 1)]
    pltpu.make_async_copy(sent, sent, back_sem).wait()


def shards(tokens, w_gate, w_up, w_down, chosen, gate_weights):
    n_tok, width = tokens.shape
    n_dev, slots = chosen.shape
    ff = w_gate.shape[2]
    n_sub = n_dev // SUB
    total = n_dev * PAIR
    return pl.pallas_call(
        body,
        out_shape=pltpu.VMEM((n_tok, width), BF),
        in_specs=[pl.BlockSpec(memory_space=pltpu.HBM)] * 6,
        out_specs=pl.BlockSpec(memory_space=pltpu.VMEM),
        scratch_shapes=[
            pltpu.VMEM((n_tok, width), BF),
            pltpu.VMEM((width, ff), BF),
            pltpu.VMEM((width, ff), BF),
            pltpu.VMEM((ff, width), BF),
            pltpu.VMEM((n_dev, slots), jnp.int32),
            pltpu.VMEM((n_dev, slots), F32),
            pltpu.VMEM((slots, slots), BF),
            pltpu.VMEM((n_dev, slots), F32),
            pltpu.VMEM((n_dev, slots), F32),
            pltpu.VMEM((n_dev, slots), F32),
            pltpu.VMEM((total, n_tok), F32),
            pltpu.VMEM((n_tok, total), BF),
            pltpu.VMEM((total, 128), F32),
            pltpu.VMEM((n_dev, PAIR, width), BF),
            pltpu.VMEM((n_dev, PAIR, width), BF),
            pltpu.VMEM((n_dev, PAIR, width), BF),
            pltpu.VMEM((n_dev, PAIR, width), BF),
            pltpu.VMEM((SUB * PAIR, ff), BF),
            pltpu.VMEM((n_tok, width), F32),
            pltpu.SemaphoreType.DMA((6,)),
            pltpu.SemaphoreType.DMA,
            pltpu.SemaphoreType.DMA((n_sub,)),
            pltpu.SemaphoreType.DMA,
            pltpu.SemaphoreType.DMA((n_sub,)),
            pltpu.SemaphoreType.REGULAR,
        ],
        compiler_params=pltpu.CompilerParams(
            collective_id=0, has_side_effects=True, vmem_limit_bytes=56 << 20
        ),
    )(tokens, w_gate, w_up, w_down, chosen, gate_weights)


def solution(mesh):
    return jax.shard_map(
        shards,
        mesh=mesh,
        in_specs=(
            P(("grp", "loc"), None),
            P(("grp", "loc"), None, None),
            P(("grp", "loc"), None, None),
            P(("grp", "loc"), None, None),
            P(),
            P(),
        ),
        out_specs=P(("grp", "loc"), None),
        check_vma=False,
    )
```

```python
import itertools

import jax
import jax.numpy as jnp
from jax import lax
from jax.experimental import pallas as pl
from jax.experimental.pallas import tpu as pltpu
from jax.sharding import PartitionSpec as P

N_FIRST = 19
PAIR = 8
SUB = 16
FF_TILES = ((0, 1024), (1024, 1024), (2048, 768))
MESH = pl.DeviceIdType.MESH
BF = jnp.bfloat16
F32 = jnp.float32


def by_link_load(offsets):
    loads = {}
    for o in offsets:
        hops = []
        for d in (o[0], o[2], o[3]):
            hops += [1.0 if d in (1, 2) else 0.0, 1.0 if d in (2, 3) else 0.0]
        loads[o] = hops
    total = [sum(loads[o][i] for o in offsets) for i in range(6)]
    left, done, out = list(offsets), [0.0] * 6, []
    for n in range(len(offsets)):
        goal = [(n + 1) * t / len(offsets) for t in total]
        best = min(left, key=lambda o: sum((a + b - g) ** 2 for a, b, g in zip(done, loads[o], goal)))
        done = [a + b for a, b in zip(done, loads[best])]
        left.remove(best)
        out.append(best)
    return out


OTHERS = [o for o in itertools.product(range(4), range(2), range(4), range(4)) if any(o)]


def lines_left(o):
    return (o[:2] != (0, 0)) + (o[2] > 0) + (o[3] > 0)


NEAR = [o for o in OTHERS if lines_left(o) < 3]
X_LINE = [o for o in OTHERS if o[2] > 0 and lines_left(o) == 1]
FIRST = by_link_load(sorted(NEAR, key=lines_left)[:N_FIRST])
ORDER = [(0, 0, 0, 0)] + FIRST + by_link_load([o for o in OTHERS if o not in FIRST])


def hops(o):
    return sum(min(d, 4 - d) for d in (o[0], o[2], o[3]))


def body(
    tokens_hbm, wg_hbm, wu_hbm, wd_hbm, chosen_hbm, weight_hbm, out_ref,
    tokens, wg, wu, wd, chosen, gates, upper, key, local, key2, select, spread, scale,
    send, recv, back, home, hidden, acc,
    in_sems, send_sem, recv_sems, back_sem, home_sems, far_sem,
):
    n_dev, slots = chosen.shape
    n_tok, width = tokens.shape
    n_sub = n_dev // SUB
    rows = SUB * PAIR
    me = lax.axis_index("grp") * lax.axis_size("loc") + lax.axis_index("loc")
    g, l = lax.axis_index("grp"), lax.axis_index("loc")
    ys = [lax.rem(lax.div(g, 2) + j, 4) * 2 for j in range(4)]
    cores = [lax.rem(g + j, 2) for j in range(2)]
    xs = [lax.rem(lax.div(l, 4) + j, 4) * 4 for j in range(4)]
    zs = [lax.rem(lax.rem(l, 4) + j, 4) for j in range(4)]

    def partner(o, sign):
        dy, dc, dx, dz = o
        return ys[(sign * dy) % 4] + cores[dc], xs[(sign * dx) % 4] + zs[(sign * dz) % 4]

    loads = [
        pltpu.make_async_copy(a, b, in_sems.at[i])
        for i, (a, b) in enumerate(
            ((chosen_hbm, chosen), (tokens_hbm, tokens), (weight_hbm, gates), (wg_hbm.at[0], wg), (wu_hbm.at[0], wu), (wd_hbm.at[0], wd))
        )
    ]
    for cp in loads[:2]:
        cp.start()
    barrier = pltpu.get_barrier_semaphore()
    for o in sorted(NEAR, key=hops, reverse=True):
        pl.semaphore_signal(barrier, inc=1, device_id=partner(o, 1), device_id_type=MESH)
    for cp in loads[2:]:
        cp.start()

    row_i = lax.broadcasted_iota(jnp.int32, (slots, slots), 0)
    col_i = lax.broadcasted_iota(jnp.int32, (slots, slots), 1)
    upper[...] = jnp.where(row_i < col_i, 1.0, 0.0).astype(BF)
    pair_i = lax.broadcasted_iota(jnp.int32, (PAIR, slots), 0).astype(F32)
    token_i = (lax.broadcasted_iota(jnp.int32, (PAIR, n_tok), 1) + 1).astype(F32)

    def ranked(hit):
        ahead = jnp.dot(hit.astype(BF), upper[...], preferred_element_type=F32)
        return jnp.where(hit > 0.5, ahead, -1.0)

    loads[0].wait()
    picks = chosen[...]
    off = picks - me * n_tok
    mine = jnp.where((off >= 0) & (off < n_tok), 1.0, 0.0)
    key[...] = ranked(mine)
    local[...] = (off + 1).astype(F32)
    loads[1].wait()

    def build(s):
        for k in range(s * SUB, (s + 1) * SUB):
            pg, pl_ = partner(ORDER[k], 1)
            e = pg * lax.axis_size("loc") + pl_
            hit = key[pl.ds(e, 1), :] == pair_i
            where = jnp.sum(jnp.where(hit, local[pl.ds(e, 1), :], 0.0), axis=1, keepdims=True)
            select[k * PAIR : (k + 1) * PAIR, :] = jnp.where(token_i == where, 1.0, 0.0)
        block = select[s * rows : (s + 1) * rows, :].astype(BF)
        picked = jnp.dot(block, tokens[...], preferred_element_type=F32)
        send[s * SUB : (s + 1) * SUB] = picked.reshape(SUB, PAIR, width).astype(BF)

    def dispatch(first, last):
        for k in range(first, last):
            pltpu.make_async_remote_copy(
                send.at[k], recv.at[k], send_sem, recv_sems.at[k // SUB],
                device_id=partner(ORDER[k], 1), device_id_type=MESH,
            ).start()

    build(0)
    recv[0] = send[0]
    pl.semaphore_wait(barrier, len(NEAR))
    for o in X_LINE:
        pl.semaphore_signal(far_sem, inc=1, device_id=partner(o, 1), device_id_type=MESH)
    dispatch(1, SUB)
    for s in range(1, n_sub):
        build(s)
        first, last, known = s * SUB, (s + 1) * SUB, len(FIRST) + 1
        if first <= known < last:
            dispatch(first, known)
            pl.semaphore_wait(far_sem, len(X_LINE))
            first = known
        dispatch(first, last)

    for s in range(n_sub):
        spread[:, s * rows : (s + 1) * rows] = select[s * rows : (s + 1) * rows, :].T.astype(BF)
    own = jnp.broadcast_to(chosen[pl.ds(me, 1), :], (n_dev, slots))
    low = lax.broadcasted_iota(jnp.int32, (n_dev, slots), 0) * n_tok
    key2[...] = ranked(jnp.where((own >= low) & (own < low + n_tok), 1.0, 0.0))
    loads[2].wait()
    own_gate = gates[pl.ds(me, 1), :]

    for k in range(n_dev):
        pg, pl_ = partner(ORDER[k], -1)
        e = pg * lax.axis_size("loc") + pl_
        hit = key2[pl.ds(e, 1), :] == pair_i
        value = jnp.sum(jnp.where(hit, own_gate, 0.0), axis=1, keepdims=True)
        scale[k * PAIR : (k + 1) * PAIR, :] = jnp.broadcast_to(value, (PAIR, scale.shape[1]))

    for cp in loads[3:]:
        cp.wait()

    def got(sems, buf, s):
        @pl.when(s == 0)
        def _():
            ref = buf.at[pl.ds(1, SUB - 1)]
            pltpu.make_async_copy(ref, ref, sems.at[0]).wait()

        @pl.when(s > 0)
        def _():
            ref = buf.at[pl.ds(s * SUB, SUB)]
            pltpu.make_async_copy(ref, ref, sems.at[s]).wait()

    def expert(s, _):
        got(recv_sems, recv, s)
        x = recv[pl.ds(s * SUB, SUB)].astype(F32).reshape(rows, width).astype(BF)
        for start, size in FF_TILES:
            gate = jnp.dot(x, wg[:, start : start + size], preferred_element_type=F32)
            up = jnp.dot(x, wu[:, start : start + size], preferred_element_type=F32)
            hidden[:, start : start + size] = (gate / (1.0 + jnp.exp(-gate)) * up).astype(BF)
        made = jnp.dot(hidden[...], wd[...], preferred_element_type=F32)
        made = made * scale[pl.ds(pl.multiple_of(s * rows, rows), rows), :1]
        back[pl.ds(s * SUB, SUB)] = made.reshape(SUB, PAIR, width).astype(BF)
        for j in range(n_sub):

            @pl.when(s == j)
            def _():
                for k in range(max(j * SUB, 1), (j + 1) * SUB):
                    pltpu.make_async_remote_copy(
                        back.at[k], home.at[k], back_sem, home_sems.at[j],
                        device_id=partner(ORDER[k], -1), device_id_type=MESH,
                    ).start()

        return 0

    lax.fori_loop(0, n_sub, expert, 0)
    home[0] = back[0]

    def part(s):
        got(home_sems, home, s)
        r = home[pl.ds(s * SUB, SUB)].astype(F32).reshape(rows, width).astype(BF)
        table = spread[:, pl.ds(pl.multiple_of(s * rows, rows), rows)]
        return jnp.dot(table, r, preferred_element_type=F32)

    def combine(s, _):
        acc[...] += part(s)
        return 0

    acc[...] = part(0)
    lax.fori_loop(1, n_sub - 1, combine, 0)
    out_ref[...] = (acc[...] + part(n_sub - 1)).astype(out_ref.dtype)
    sent = send.at[pl.ds(1, n_dev - 1)]
    pltpu.make_async_copy(sent, sent, send_sem).wait()
    sent = back.at[pl.ds(1, n_dev - 1)]
    pltpu.make_async_copy(sent, sent, back_sem).wait()


def shards(tokens, w_gate, w_up, w_down, chosen, gate_weights):
    n_tok, width = tokens.shape
    n_dev, slots = chosen.shape
    ff = w_gate.shape[2]
    n_sub = n_dev // SUB
    total = n_dev * PAIR
    return pl.pallas_call(
        body,
        out_shape=pltpu.VMEM((n_tok, width), BF),
        in_specs=[pl.BlockSpec(memory_space=pltpu.HBM)] * 6,
        out_specs=pl.BlockSpec(memory_space=pltpu.VMEM),
        scratch_shapes=[
            pltpu.VMEM((n_tok, width), BF),
            pltpu.VMEM((width, ff), BF),
            pltpu.VMEM((width, ff), BF),
            pltpu.VMEM((ff, width), BF),
            pltpu.VMEM((n_dev, slots), jnp.int32),
            pltpu.VMEM((n_dev, slots), F32),
            pltpu.VMEM((slots, slots), BF),
            pltpu.VMEM((n_dev, slots), F32),
            pltpu.VMEM((n_dev, slots), F32),
            pltpu.VMEM((n_dev, slots), F32),
            pltpu.VMEM((total, n_tok), F32),
            pltpu.VMEM((n_tok, total), BF),
            pltpu.VMEM((total, 128), F32),
            pltpu.VMEM((n_dev, PAIR, width), BF),
            pltpu.VMEM((n_dev, PAIR, width), BF),
            pltpu.VMEM((n_dev, PAIR, width), BF),
            pltpu.VMEM((n_dev, PAIR, width), BF),
            pltpu.VMEM((SUB * PAIR, ff), BF),
            pltpu.VMEM((n_tok, width), F32),
            pltpu.SemaphoreType.DMA((6,)),
            pltpu.SemaphoreType.DMA,
            pltpu.SemaphoreType.DMA((n_sub,)),
            pltpu.SemaphoreType.DMA,
            pltpu.SemaphoreType.DMA((n_sub,)),
            pltpu.SemaphoreType.REGULAR,
        ],
        compiler_params=pltpu.CompilerParams(
            collective_id=0, has_side_effects=True, vmem_limit_bytes=56 << 20
        ),
    )(tokens, w_gate, w_up, w_down, chosen, gate_weights)


def solution(mesh):
    return jax.shard_map(
        shards,
        mesh=mesh,
        in_specs=(
            P(("grp", "loc"), None),
            P(("grp", "loc"), None, None),
            P(("grp", "loc"), None, None),
            P(("grp", "loc"), None, None),
            P(),
            P(),
        ),
        out_specs=P(("grp", "loc"), None),
        check_vma=False,
    )
```

```python
import itertools

import jax
import jax.numpy as jnp
from jax import lax
from jax.experimental import pallas as pl
from jax.experimental.pallas import tpu as pltpu
from jax.sharding import PartitionSpec as P

N_FIRST = 19
PAIR = 8
SUB = 16
FF_TILES = ((0, 1024), (1024, 1024), (2048, 768))
MESH = pl.DeviceIdType.MESH
BF = jnp.bfloat16
F32 = jnp.float32


def by_link_load(offsets):
    loads = {}
    for o in offsets:
        hops = []
        for d in (o[0], o[2], o[3]):
            hops += [1.0 if d in (1, 2) else 0.0, 1.0 if d in (2, 3) else 0.0]
        loads[o] = hops
    total = [sum(loads[o][i] for o in offsets) for i in range(6)]
    left, done, out = list(offsets), [0.0] * 6, []
    for n in range(len(offsets)):
        goal = [(n + 1) * t / len(offsets) for t in total]
        best = min(left, key=lambda o: sum((a + b - g) ** 2 for a, b, g in zip(done, loads[o], goal)))
        done = [a + b for a, b in zip(done, loads[best])]
        left.remove(best)
        out.append(best)
    return out


OTHERS = [o for o in itertools.product(range(4), range(2), range(4), range(4)) if any(o)]


def lines_left(o):
    return (o[:2] != (0, 0)) + (o[2] > 0) + (o[3] > 0)


NEAR = [o for o in OTHERS if lines_left(o) < 3]
X_LINE = [o for o in OTHERS if o[2] > 0 and lines_left(o) == 1]
FIRST = by_link_load(sorted(NEAR, key=lines_left)[:N_FIRST])
ORDER = [(0, 0, 0, 0)] + FIRST + by_link_load([o for o in OTHERS if o not in FIRST])


def hops(o):
    return sum(min(d, 4 - d) for d in (o[0], o[2], o[3]))


def body(
    tokens_hbm, wg_hbm, wu_hbm, wd_hbm, chosen_hbm, weight_hbm, out_ref,
    tokens, wg, wu, wd, chosen, gates, upper, key, local, key2, select, spread, scale,
    send, recv, back, home, hidden, acc,
    in_sems, send_sem, recv_sems, back_sem, home_sems, far_sem,
):
    n_dev, slots = chosen.shape
    n_tok, width = tokens.shape
    n_sub = n_dev // SUB
    rows = SUB * PAIR
    me = lax.axis_index("grp") * lax.axis_size("loc") + lax.axis_index("loc")
    g, l = lax.axis_index("grp"), lax.axis_index("loc")
    ys = [lax.rem(lax.div(g, 2) + j, 4) * 2 for j in range(4)]
    cores = [lax.rem(g + j, 2) for j in range(2)]
    xs = [lax.rem(lax.div(l, 4) + j, 4) * 4 for j in range(4)]
    zs = [lax.rem(lax.rem(l, 4) + j, 4) for j in range(4)]

    def partner(o, sign):
        dy, dc, dx, dz = o
        return ys[(sign * dy) % 4] + cores[dc], xs[(sign * dx) % 4] + zs[(sign * dz) % 4]

    barrier = pltpu.get_barrier_semaphore()
    for o in sorted(NEAR, key=hops, reverse=True):
        pl.semaphore_signal(barrier, inc=1, device_id=partner(o, 1), device_id_type=MESH)
    loads = [
        pltpu.make_async_copy(a, b, in_sems.at[i])
        for i, (a, b) in enumerate(
            ((chosen_hbm, chosen), (tokens_hbm, tokens), (weight_hbm, gates), (wg_hbm.at[0], wg), (wu_hbm.at[0], wu), (wd_hbm.at[0], wd))
        )
    ]
    for cp in loads[:3]:
        cp.start()

    row_i = lax.broadcasted_iota(jnp.int32, (slots, slots), 0)
    col_i = lax.broadcasted_iota(jnp.int32, (slots, slots), 1)
    upper[...] = jnp.where(row_i < col_i, 1.0, 0.0).astype(BF)
    pair_i = lax.broadcasted_iota(jnp.int32, (PAIR, slots), 0).astype(F32)
    token_i = (lax.broadcasted_iota(jnp.int32, (PAIR, n_tok), 1) + 1).astype(F32)

    def ranked(hit):
        ahead = jnp.dot(hit.astype(BF), upper[...], preferred_element_type=F32)
        return jnp.where(hit > 0.5, ahead, -1.0)

    loads[0].wait()
    picks = chosen[...]
    off = picks - me * n_tok
    mine = jnp.where((off >= 0) & (off < n_tok), 1.0, 0.0)
    key[...] = ranked(mine)
    local[...] = (off + 1).astype(F32)
    loads[1].wait()

    def build(s):
        for k in range(s * SUB, (s + 1) * SUB):
            pg, pl_ = partner(ORDER[k], 1)
            e = pg * lax.axis_size("loc") + pl_
            hit = key[pl.ds(e, 1), :] == pair_i
            where = jnp.sum(jnp.where(hit, local[pl.ds(e, 1), :], 0.0), axis=1, keepdims=True)
            select[k * PAIR : (k + 1) * PAIR, :] = jnp.where(token_i == where, 1.0, 0.0)
        block = select[s * rows : (s + 1) * rows, :].astype(BF)
        picked = jnp.dot(block, tokens[...], preferred_element_type=F32)
        send[s * SUB : (s + 1) * SUB] = picked.reshape(SUB, PAIR, width).astype(BF)

    def dispatch(first, last):
        for k in range(first, last):
            pltpu.make_async_remote_copy(
                send.at[k], recv.at[k], send_sem, recv_sems.at[k // SUB],
                device_id=partner(ORDER[k], 1), device_id_type=MESH,
            ).start()

    build(0)
    recv[0] = send[0]
    for cp in loads[3:]:
        cp.start()
    pl.semaphore_wait(barrier, len(NEAR))
    for o in X_LINE:
        pl.semaphore_signal(far_sem, inc=1, device_id=partner(o, 1), device_id_type=MESH)
    dispatch(1, SUB)
    for s in range(1, n_sub):
        build(s)
        first, last, known = s * SUB, (s + 1) * SUB, len(FIRST) + 1
        if first <= known < last:
            dispatch(first, known)
            pl.semaphore_wait(far_sem, len(X_LINE))
            first = known
        dispatch(first, last)

    for s in range(n_sub):
        spread[:, s * rows : (s + 1) * rows] = select[s * rows : (s + 1) * rows, :].T.astype(BF)
    own = jnp.broadcast_to(chosen[pl.ds(me, 1), :], (n_dev, slots))
    low = lax.broadcasted_iota(jnp.int32, (n_dev, slots), 0) * n_tok
    key2[...] = ranked(jnp.where((own >= low) & (own < low + n_tok), 1.0, 0.0))
    loads[2].wait()
    own_gate = gates[pl.ds(me, 1), :]

    for k in range(n_dev):
        pg, pl_ = partner(ORDER[k], -1)
        e = pg * lax.axis_size("loc") + pl_
        hit = key2[pl.ds(e, 1), :] == pair_i
        value = jnp.sum(jnp.where(hit, own_gate, 0.0), axis=1, keepdims=True)
        scale[k * PAIR : (k + 1) * PAIR, :] = jnp.broadcast_to(value, (PAIR, scale.shape[1]))

    for cp in loads[3:]:
        cp.wait()

    def got(sems, buf, s):
        @pl.when(s == 0)
        def _():
            ref = buf.at[pl.ds(1, SUB - 1)]
            pltpu.make_async_copy(ref, ref, sems.at[0]).wait()

        @pl.when(s > 0)
        def _():
            ref = buf.at[pl.ds(s * SUB, SUB)]
            pltpu.make_async_copy(ref, ref, sems.at[s]).wait()

    def expert(s, _):
        got(recv_sems, recv, s)
        x = recv[pl.ds(s * SUB, SUB)].astype(F32).reshape(rows, width).astype(BF)
        for start, size in FF_TILES:
            gate = jnp.dot(x, wg[:, start : start + size], preferred_element_type=F32)
            up = jnp.dot(x, wu[:, start : start + size], preferred_element_type=F32)
            hidden[:, start : start + size] = (gate / (1.0 + jnp.exp(-gate)) * up).astype(BF)
        made = jnp.dot(hidden[...], wd[...], preferred_element_type=F32)
        made = made * scale[pl.ds(pl.multiple_of(s * rows, rows), rows), :1]
        back[pl.ds(s * SUB, SUB)] = made.reshape(SUB, PAIR, width).astype(BF)
        for j in range(n_sub):

            @pl.when(s == j)
            def _():
                for k in range(max(j * SUB, 1), (j + 1) * SUB):
                    pltpu.make_async_remote_copy(
                        back.at[k], home.at[k], back_sem, home_sems.at[j],
                        device_id=partner(ORDER[k], -1), device_id_type=MESH,
                    ).start()

        return 0

    lax.fori_loop(0, n_sub, expert, 0)
    home[0] = back[0]
    acc[...] = jnp.zeros_like(acc)

    def part(s):
        got(home_sems, home, s)
        r = home[pl.ds(s * SUB, SUB)].astype(F32).reshape(rows, width).astype(BF)
        table = spread[:, pl.ds(pl.multiple_of(s * rows, rows), rows)]
        return jnp.dot(table, r, preferred_element_type=F32)

    def combine(s, _):
        acc[...] += part(s)
        return 0

    lax.fori_loop(0, n_sub - 1, combine, 0)
    out_ref[...] = (acc[...] + part(n_sub - 1)).astype(out_ref.dtype)
    sent = send.at[pl.ds(1, n_dev - 1)]
    pltpu.make_async_copy(sent, sent, send_sem).wait()
    sent = back.at[pl.ds(1, n_dev - 1)]
    pltpu.make_async_copy(sent, sent, back_sem).wait()


def shards(tokens, w_gate, w_up, w_down, chosen, gate_weights):
    n_tok, width = tokens.shape
    n_dev, slots = chosen.shape
    ff = w_gate.shape[2]
    n_sub = n_dev // SUB
    total = n_dev * PAIR
    return pl.pallas_call(
        body,
        out_shape=pltpu.VMEM((n_tok, width), BF),
        in_specs=[pl.BlockSpec(memory_space=pltpu.HBM)] * 6,
        out_specs=pl.BlockSpec(memory_space=pltpu.VMEM),
        scratch_shapes=[
            pltpu.VMEM((n_tok, width), BF),
            pltpu.VMEM((width, ff), BF),
            pltpu.VMEM((width, ff), BF),
            pltpu.VMEM((ff, width), BF),
            pltpu.VMEM((n_dev, slots), jnp.int32),
            pltpu.VMEM((n_dev, slots), F32),
            pltpu.VMEM((slots, slots), BF),
            pltpu.VMEM((n_dev, slots), F32),
            pltpu.VMEM((n_dev, slots), F32),
            pltpu.VMEM((n_dev, slots), F32),
            pltpu.VMEM((total, n_tok), F32),
            pltpu.VMEM((n_tok, total), BF),
            pltpu.VMEM((total, 128), F32),
            pltpu.VMEM((n_dev, PAIR, width), BF),
            pltpu.VMEM((n_dev, PAIR, width), BF),
            pltpu.VMEM((n_dev, PAIR, width), BF),
            pltpu.VMEM((n_dev, PAIR, width), BF),
            pltpu.VMEM((SUB * PAIR, ff), BF),
            pltpu.VMEM((n_tok, width), F32),
            pltpu.SemaphoreType.DMA((6,)),
            pltpu.SemaphoreType.DMA,
            pltpu.SemaphoreType.DMA((n_sub,)),
            pltpu.SemaphoreType.DMA,
            pltpu.SemaphoreType.DMA((n_sub,)),
            pltpu.SemaphoreType.REGULAR,
        ],
        compiler_params=pltpu.CompilerParams(
            collective_id=0, has_side_effects=True, vmem_limit_bytes=56 << 20
        ),
    )(tokens, w_gate, w_up, w_down, chosen, gate_weights)


def solution(mesh):
    return jax.shard_map(
        shards,
        mesh=mesh,
        in_specs=(
            P(("grp", "loc"), None),
            P(("grp", "loc"), None, None),
            P(("grp", "loc"), None, None),
            P(("grp", "loc"), None, None),
            P(),
            P(),
        ),
        out_specs=P(("grp", "loc"), None),
        check_vma=False,
    )
```
